32 devices in a mesh: seq: 8 (over z, core), head: 4 (over y, x).
Axes of the slice: x: 2, y: 2, z: 4, core: 2. Of those that a mesh axis runs over, the one named last changes fastest.
Arguments:
- queries: bfloat16 [4096, 1024], P('seq', 'head'), may hold values from -6 to 6
- keys: bfloat16 [4096, 256], P(('seq', 'head')), may hold values from -6 to 6
- values: bfloat16 [4096, 256], P(('seq', 'head')), may hold values from -3 to 3
- attn_out: bfloat16 [4096, 1024], P('seq', 'head'), may hold values from -1.796875 to 1.796875
- out_grad: bfloat16 [4096, 1024], P('seq', 'head'), may hold values from -6 to 6
- log_norm: float32 [8, 4096], P('head', 'seq'), may hold values from 3.5 to 5.5
- block_layout: int32 [8, 32, 32], P('head'), may hold values 0 or 1
- document_ids: int32 [4096], replicated, may hold values from 0 to 7, never falling along the last dimension, each value on 1 to 2048 neighbouring positions
- block_order: int32 [32], replicated, may hold values from 0 to 31, each once
Outputs:
- query_grad: float32 [4096, 1024], P('seq', 'head')
- key_grad: float32 [4096, 256], P(('seq', 'head'))
- value_grad: float32 [4096, 256], P(('seq', 'head'))
The draws below stay inside these ranges and needn't reach their ends.
Inputs may be any that keep to these rules, and one draw needn't show every extreme that they name: `document_ids`: never falls along the sequence position; each document covers 1 to 2048 positions, one exactly 2048. `block_order`: each sequence block once.
All inputs are finite; a program needn't handle non-finite values.
Results may differ from the reference program's by a relative error of at most 0.0029.
Values may be sent and summed in bfloat16 or wider, within the bound.
A program may use at most 128 MiB of HBM per device.

```python
import math
import jax
import jax.numpy as jnp
import numpy as np
from jax import lax

D_HEAD = 128
GROUP = 4
BLOCK = 128
DOCS = 8
HEADS = 8
KV_HEADS = 2
SEQ = 4096
NBLK = 32


def touch_ends(entries, stream_key, low, largest):
    longest = entries.shape.index(max(entries.shape))
    spots = []
    for shift in (0, 1):
        where = [jax.random.randint(jax.random.fold_in(stream_key, axis), (), 0, length) for axis, length in enumerate(entries.shape)]
        where[longest] = (where[longest] + shift) % entries.shape[longest]
        spots.append(tuple(where))
    return entries.at[spots[0]].set(low).at[spots[1]].set(largest)


def steps_of(key, dims, shards, smallest, high):
    def one(axis_at, parts):
        heights = jax.random.uniform(jax.random.fold_in(jax.random.fold_in(key, 6), axis_at), (parts,), jnp.float32, smallest / len(shards), high / len(shards))
        return jnp.repeat(jnp.exp(heights), dims[axis_at] // parts).reshape((-1,) + (1,) * (len(dims) - axis_at - 1))

    loudness = one(*shards[0])
    for cut in shards[1:]:
        loudness = loudness * one(*cut)
    return loudness


def split_up(count, total, most, lean):
    loads = [(1 << 20) // math.isqrt(grade ** lean) + 1 for grade in range(2, count + 1)]
    surplus, counts = total - most - (count - 1), [1] * (count - 1)
    while surplus > 0:
        movable = [i for i in range(count - 1) if counts[i] < most]
        mass, budget = sum([loads[i] for i in movable]), surplus
        for i in movable:
            addition = min(most - counts[i], max(1, budget * loads[i] // mass), surplus)
            counts[i] = counts[i] + addition
            surplus = surplus - addition
    return np.array([most] + counts)


def uneven_parts(own_key, number_of, total, most, skew):
    if number_of == 2:
        one = jax.random.randint(own_key, (), max(1, total - most), min(most, total - 1) + 1)
        return jnp.stack([one, total - one])
    tallies = jnp.asarray(split_up(number_of, total, most, skew), jnp.int32)
    pairs = (number_of - 1) // 2
    source_of, taker = tallies[1:1 + 2 * pairs:2], tallies[2:2 + 2 * pairs:2]
    margin = jnp.minimum(source_of - 1, most - taker)
    shifted = jax.random.randint(jax.random.fold_in(own_key, 1), (pairs,), 0, 1 << 20) % (margin + 1)
    tallies = tallies.at[1:1 + 2 * pairs:2].set(source_of - shifted).at[2:2 + 2 * pairs:2].set(taker + shifted)
    return tallies[jax.random.permutation(jax.random.fold_in(own_key, 2), number_of)]


def bell_draw(key, shape, spread, reach, split=(), kind=jnp.bfloat16):
    drawn = spread * jax.random.normal(key, shape, jnp.float32)
    if split:
        drawn = drawn * steps_of(key, shape, split, -0.22, 0.18)
    return jnp.clip(drawn, -reach, reach).astype(kind)


def setup_inputs(seed: int = 0) -> dict:
    arg_keys = jax.random.split(jax.random.key(seed), 10)
    return {
        "queries": bell_draw(arg_keys[0], (SEQ, HEADS * D_HEAD), 1.0, 6.0, ((0, 8), (1, 4))),
        "keys": bell_draw(arg_keys[1], (SEQ, KV_HEADS * D_HEAD), 1.0, 6.0, ((0, 32),)),
        "values": bell_draw(arg_keys[2], (SEQ, KV_HEADS * D_HEAD), 0.5, 3.0, ((0, 32),)),
        "attn_out": bell_draw(arg_keys[3], (SEQ, HEADS * D_HEAD), 0.3, 1.796875, ((0, 8), (1, 4))),
        "out_grad": bell_draw(arg_keys[4], (SEQ, HEADS * D_HEAD), 1.0, 6.0, ((0, 8), (1, 4))),
        "log_norm": jnp.clip(3.5 + 2.0 * jax.random.uniform(arg_keys[5], (HEADS, SEQ), jnp.float32) ** steps_of(arg_keys[5], (HEADS, SEQ), ((0, 4), (1, 8)), -0.2, 0.2), 3.5, 5.5),
        "block_layout": touch_ends((jax.random.randint(arg_keys[6], (HEADS, NBLK, NBLK), 0, 4) < 3).astype(jnp.int32), jax.random.fold_in(arg_keys[6], 1), 0, 1),
        "document_ids": jnp.searchsorted(jnp.cumsum(uneven_parts(arg_keys[7], DOCS, SEQ, SEQ // 2, 2)), jnp.arange(SEQ), side="right").astype(jnp.int32),
        "block_order": jax.random.permutation(arg_keys[8], NBLK).astype(jnp.int32),
    }


def stored_positions(block_order, document_ids):
    stored = jnp.arange(SEQ, dtype=jnp.int32)
    position = block_order[stored // BLOCK].astype(jnp.int32) * BLOCK + stored % BLOCK
    return position, document_ids[position]


def reference(queries, keys, values, attn_out, out_grad, log_norm, block_layout, document_ids, block_order):
    position, docs = stored_positions(block_order, document_ids)
    blocks = position // BLOCK
    scaling = D_HEAD ** -0.5
    allowed = (position[None, :] <= position[:, None]) & (docs[:, None] == docs[None, :])
    query_heads = queries.reshape(SEQ, HEADS, D_HEAD).transpose(1, 0, 2)
    grad_heads = out_grad.reshape(SEQ, HEADS, D_HEAD).transpose(1, 0, 2)
    out_heads = attn_out.reshape(SEQ, HEADS, D_HEAD).transpose(1, 0, 2)
    key_heads = keys.reshape(SEQ, KV_HEADS, D_HEAD).transpose(1, 0, 2)
    value_heads = values.reshape(SEQ, KV_HEADS, D_HEAD).transpose(1, 0, 2)

    def one_head(head_index):
        query_one = query_heads[head_index]
        grad_one = grad_heads[head_index]
        out_one = out_heads[head_index]
        key_one = key_heads[head_index // GROUP]
        value_one = value_heads[head_index // GROUP]
        layout_one = block_layout[head_index][blocks[:, None], blocks[None, :]] == 1
        visible = allowed & layout_one
        scores = jnp.dot(query_one, key_one.T, preferred_element_type=jnp.float32) * scaling
        weights = jnp.where(visible, jnp.exp(scores - log_norm[head_index][:, None]), 0.0)
        weights_low = weights.astype(jnp.bfloat16)
        value_part = jnp.dot(weights_low.T, grad_one, preferred_element_type=jnp.float32)
        grad_scores = jnp.dot(grad_one, value_one.T, preferred_element_type=jnp.float32)
        delta = jnp.sum(grad_one.astype(jnp.float32) * out_one.astype(jnp.float32), axis=1)
        score_grad = (weights * (grad_scores - delta[:, None])).astype(jnp.bfloat16)
        query_part = jnp.dot(score_grad, key_one, preferred_element_type=jnp.float32)
        key_part = jnp.dot(score_grad.T, query_one, preferred_element_type=jnp.float32)
        return query_part, key_part, value_part

    query_all, key_all, value_all = lax.map(one_head, jnp.arange(HEADS, dtype=jnp.int32))
    query_grad = (query_all * scaling).transpose(1, 0, 2).reshape(SEQ, HEADS * D_HEAD)
    key_sum = key_all.reshape(KV_HEADS, GROUP, SEQ, D_HEAD).sum(axis=1) * scaling
    value_sum = value_all.reshape(KV_HEADS, GROUP, SEQ, D_HEAD).sum(axis=1)
    key_grad = key_sum.transpose(1, 0, 2).reshape(SEQ, KV_HEADS * D_HEAD)
    value_grad = value_sum.transpose(1, 0, 2).reshape(SEQ, KV_HEADS * D_HEAD)
    return (query_grad, key_grad, value_grad)
```

```python
import functools
import math

import jax
import jax.numpy as jnp
from jax import lax
from jax.experimental import pallas as pl
from jax.experimental.pallas import tpu as pltpu
from jax.sharding import PartitionSpec as P

D_HEAD = 128
GROUP = 4
BLOCK = 128
DOCS = 8
CHUNK = 4
LOG2E = math.log2(math.e)
NT = (((1,), (1,)), ((), ()))
TN = (((0,), (0,)), ((), ()))


def grads_kernel(
    order, first, starts, layout, docs, q_ref, do_ref, o_ref, ln_ref, kv_ref,
    dq_ref, dkv_ref, acc, inverse, dqt,
):
    heads = ln_ref.shape[0]
    blocks = order.shape[0]
    own = q_ref.shape[0] // BLOCK
    scale = D_HEAD ** -0.5
    me = lax.axis_index("seq")
    wide = heads * BLOCK

    def clear(r, _):
        inverse[order[r]] = r
        acc[pl.ds(r * BLOCK, BLOCK), :] = jnp.zeros((BLOCK, 2 * D_HEAD), jnp.float32)
        return 0

    lax.fori_loop(0, blocks, clear, 0)
    lane = lax.broadcasted_iota(jnp.int32, (1, wide), 1)
    sub = lax.broadcasted_iota(jnp.int32, (BLOCK, wide), 0)

    def per_query_block(i, _):
        rows = pl.ds(i * BLOCK, BLOCK)
        qb = order[me * own + i]
        ids = docs[pl.ds(qb, 1), :]
        low = jnp.zeros((1, BLOCK), jnp.int32)
        for d in range(1, DOCS):
            low = jnp.where(ids >= d, starts[d], low)
        low = jnp.concatenate([low] * heads, axis=1)
        high = qb * BLOCK + lane % BLOCK
        q2 = jnp.concatenate(
            [q_ref[rows, h * D_HEAD:(h + 1) * D_HEAD] for h in range(heads)], axis=0)
        do2 = jnp.concatenate(
            [do_ref[rows, h * D_HEAD:(h + 1) * D_HEAD] for h in range(heads)], axis=0)
        o2 = jnp.concatenate(
            [o_ref[rows, h * D_HEAD:(h + 1) * D_HEAD] for h in range(heads)], axis=0)
        product = do2.astype(jnp.float32) * o2.astype(jnp.float32)
        delta = jnp.sum(product.T, axis=0, keepdims=True)
        norm = jnp.concatenate([ln_ref[h:h + 1, rows] for h in range(heads)], axis=1) * LOG2E
        dqt[...] = jnp.zeros_like(dqt)
        begin = first[qb]
        trips = (qb - begin + CHUNK) // CHUNK

        def per_chunk(t, _):
            slots, keeps, ks, vs = [], [], [], []
            for c in range(CHUNK):
                kb = begin + t * CHUNK + c
                held = jnp.minimum(kb, qb)
                slot = pl.multiple_of(inverse[held] * BLOCK, BLOCK)
                slots.append(slot)
                top = jnp.full((1, wide), -1, jnp.int32)
                for h in range(heads):
                    on = (layout[(h * blocks + qb) * blocks + held] == 1) & (kb <= qb)
                    limit = jnp.where(on, 1 << 30, -1)
                    top = jnp.where(lane // BLOCK == h, jnp.minimum(high, limit), top)
                keeps.append((sub >= low - held * BLOCK) & (sub <= top - held * BLOCK))
                ks.append(kv_ref[pl.ds(slot, BLOCK), :D_HEAD])
                vs.append(kv_ref[pl.ds(slot, BLOCK), D_HEAD:])
            k4 = jnp.concatenate(ks, axis=0)
            v4 = jnp.concatenate(vs, axis=0)
            keep = jnp.concatenate(keeps, axis=0)
            st = lax.dot_general(k4, q2, NT, preferred_element_type=jnp.float32)
            dpt = lax.dot_general(v4, do2, NT, preferred_element_type=jnp.float32)
            w = jnp.where(keep, jnp.exp2(st * (scale * LOG2E) - norm), 0.0)
            wl = w.astype(jnp.bfloat16)
            dv = jnp.dot(wl, do2, preferred_element_type=jnp.float32)
            ds = (w * (dpt - delta)).astype(jnp.bfloat16)
            dk = jnp.dot(ds, q2, preferred_element_type=jnp.float32)
            dqt[...] += lax.dot_general(k4, ds, TN, preferred_element_type=jnp.float32)
            for c in range(CHUNK):
                part = slice(c * BLOCK, (c + 1) * BLOCK)
                acc[pl.ds(slots[c], BLOCK), :D_HEAD] += dk[part]
                acc[pl.ds(slots[c], BLOCK), D_HEAD:] += dv[part]
            return 0

        lax.fori_loop(0, trips, per_chunk, 0)
        for h in range(heads):
            dq_ref[rows, h * D_HEAD:(h + 1) * D_HEAD] = (
                dqt[:, h * BLOCK:(h + 1) * BLOCK].T * scale)
        return 0

    lax.fori_loop(0, own, per_query_block, 0)

    def finish(r, _):
        rows = pl.ds(r * BLOCK, BLOCK)
        dkv_ref[rows, :D_HEAD] = (acc[rows, :D_HEAD] * scale).astype(dkv_ref.dtype)
        dkv_ref[rows, D_HEAD:] = acc[rows, D_HEAD:].astype(dkv_ref.dtype)
        return 0

    lax.fori_loop(0, blocks, finish, 0)


def local_grads(queries, out_grad, attn_out, log_norm, kv_all, block_layout, document_ids,
                block_order, sum_type):
    blocks = block_order.shape[0]
    total = kv_all.shape[0]
    starts = jnp.sum(
        (document_ids[None, :] < jnp.arange(DOCS, dtype=jnp.int32)[:, None]).astype(jnp.int32),
        axis=1)
    heads_of = document_ids.reshape(blocks, BLOCK)
    first_ids = heads_of[:, 0]
    first = jnp.sum(
        (document_ids[None, :] < first_ids[:, None]).astype(jnp.int32), axis=1) // BLOCK
    smem = pl.BlockSpec(memory_space=pltpu.SMEM)
    vmem = pl.BlockSpec(memory_space=pltpu.VMEM)
    heads = log_norm.shape[0]
    return pl.pallas_call(
        grads_kernel,
        out_shape=(
            jax.ShapeDtypeStruct(queries.shape, jnp.float32),
            jax.ShapeDtypeStruct((total, 2 * D_HEAD), sum_type),
        ),
        in_specs=[smem] * 4 + [vmem] * 6,
        out_specs=(vmem, vmem),
        scratch_shapes=[
            pltpu.VMEM((total, 2 * D_HEAD), jnp.float32),
            pltpu.SMEM((blocks,), jnp.int32),
            pltpu.VMEM((D_HEAD, heads * BLOCK), jnp.float32),
        ],
        name="grads",
    )(block_order, first, starts, block_layout.reshape(-1), heads_of,
      queries, out_grad, attn_out, log_norm, kv_all)


def body(
    queries, keys, values, attn_out, out_grad, log_norm, block_layout, document_ids, block_order
):
    rows = keys.shape[0]
    heads = log_norm.shape[0]
    kv_heads = keys.shape[1] // D_HEAD
    repeats = GROUP // heads
    pair = jnp.concatenate(
        [keys.reshape(rows, kv_heads, D_HEAD), values.reshape(rows, kv_heads, D_HEAD)], axis=2)
    pair = jnp.broadcast_to(pair[:, :, None, :], (rows, kv_heads, repeats, 2 * D_HEAD))
    pair = lax.all_to_all(
        pair.reshape(rows, -1), "head", split_axis=1, concat_axis=0, tiled=True)
    kv_all = lax.all_gather(pair, "seq", axis=0, tiled=True)
    dq, dkv = local_grads(queries, out_grad, attn_out, log_norm, kv_all, block_layout,
                          document_ids, block_order, jnp.float32)
    dkv = lax.psum_scatter(dkv, "seq", scatter_dimension=0, tiled=True)
    dkv = lax.all_to_all(dkv, "head", split_axis=0, concat_axis=1, tiled=True)
    dkv = dkv.reshape(rows, kv_heads, repeats, 2, D_HEAD).sum(axis=2)
    return (dq, dkv[:, :, 0].reshape(rows, -1), dkv[:, :, 1].reshape(rows, -1))


def solution(mesh):
    in_specs = (
        P("seq", "head"),
        P(("seq", "head"), None),
        P(("seq", "head"), None),
        P("seq", "head"),
        P("seq", "head"),
        P("head", "seq"),
        P("head", None, None),
        P(),
        P(),
    )
    out_specs = (P("seq", "head"), P(("seq", "head"), None), P(("seq", "head"), None))
    return jax.shard_map(body, mesh=mesh, in_specs=in_specs, out_specs=out_specs, check_vma=False)
```

```python
import functools
import math

import jax
import jax.numpy as jnp
from jax import lax
from jax.experimental import pallas as pl
from jax.experimental.pallas import tpu as pltpu
from jax.sharding import PartitionSpec as P

D_HEAD = 128
GROUP = 4
BLOCK = 128
DOCS = 8
CHUNK = 4
LOG2E = math.log2(math.e)
NT = (((1,), (1,)), ((), ()))
TN = (((0,), (0,)), ((), ()))


def grads_kernel(
    order, first, starts, layout, docs, q_ref, do_ref, o_ref, ln_ref, kv_ref,
    dq_ref, dkv_ref, acc, inverse, dqt,
):
    heads = ln_ref.shape[0]
    blocks = order.shape[0]
    own = q_ref.shape[0] // BLOCK
    scale = D_HEAD ** -0.5
    me = lax.axis_index("seq")
    wide = heads * BLOCK

    def clear(r, _):
        inverse[order[r]] = r
        acc[:, pl.ds(r * BLOCK, BLOCK), :] = jnp.zeros((2, BLOCK, D_HEAD), jnp.float32)
        return 0

    lax.fori_loop(0, blocks, clear, 0)
    lane = lax.broadcasted_iota(jnp.int32, (1, wide), 1)
    sub = lax.broadcasted_iota(jnp.int32, (BLOCK, wide), 0)

    def per_query_block(i, _):
        rows = pl.ds(i * BLOCK, BLOCK)
        qb = order[me * own + i]
        ids = docs[pl.ds(qb, 1), :]
        low = jnp.zeros((1, BLOCK), jnp.int32)
        for d in range(1, DOCS):
            low = jnp.where(ids >= d, starts[d], low)
        low = jnp.concatenate([low] * heads, axis=1)
        high = qb * BLOCK + lane % BLOCK
        q2 = jnp.concatenate(
            [q_ref[rows, h * D_HEAD:(h + 1) * D_HEAD] for h in range(heads)], axis=0)
        do2 = jnp.concatenate(
            [do_ref[rows, h * D_HEAD:(h + 1) * D_HEAD] for h in range(heads)], axis=0)
        o2 = jnp.concatenate(
            [o_ref[rows, h * D_HEAD:(h + 1) * D_HEAD] for h in range(heads)], axis=0)
        product = do2.astype(jnp.float32) * o2.astype(jnp.float32)
        delta = jnp.sum(product.T, axis=0, keepdims=True)
        norm = jnp.concatenate([ln_ref[h:h + 1, rows] for h in range(heads)], axis=1) * LOG2E
        dqt[...] = jnp.zeros_like(dqt)
        begin = first[qb]
        trips = (qb - begin + CHUNK) // CHUNK

        def per_chunk(t, _):
            slots, keeps, ks, vs = [], [], [], []
            for c in range(CHUNK):
                kb = begin + t * CHUNK + c
                held = jnp.minimum(kb, qb)
                slot = pl.multiple_of(inverse[held] * BLOCK, BLOCK)
                slots.append(slot)
                top = jnp.full((1, wide), -1, jnp.int32)
                for h in range(heads):
                    on = (layout[(h * blocks + qb) * blocks + held] == 1) & (kb <= qb)
                    limit = jnp.where(on, 1 << 30, -1)
                    top = jnp.where(lane // BLOCK == h, jnp.minimum(high, limit), top)
                keeps.append((sub >= low - held * BLOCK) & (sub <= top - held * BLOCK))
                ks.append(kv_ref[0, pl.ds(slot, BLOCK), :])
                vs.append(kv_ref[1, pl.ds(slot, BLOCK), :])
            k4 = jnp.concatenate(ks, axis=0)
            v4 = jnp.concatenate(vs, axis=0)
            keep = jnp.concatenate(keeps, axis=0)
            st = lax.dot_general(k4, q2, NT, preferred_element_type=jnp.float32)
            dpt = lax.dot_general(v4, do2, NT, preferred_element_type=jnp.float32)
            w = jnp.where(keep, jnp.exp2(st * (scale * LOG2E) - norm), 0.0)
            wl = w.astype(jnp.bfloat16)
            dv = jnp.dot(wl, do2, preferred_element_type=jnp.float32)
            ds = (w * (dpt - delta)).astype(jnp.bfloat16)
            dk = jnp.dot(ds, q2, preferred_element_type=jnp.float32)
            dqt[...] += lax.dot_general(k4, ds, TN, preferred_element_type=jnp.float32)
            for c in range(CHUNK):
                part = slice(c * BLOCK, (c + 1) * BLOCK)
                acc[0, pl.ds(slots[c], BLOCK), :] += dk[part]
                acc[1, pl.ds(slots[c], BLOCK), :] += dv[part]
            return 0

        lax.fori_loop(0, trips, per_chunk, 0)
        for h in range(heads):
            dq_ref[rows, h * D_HEAD:(h + 1) * D_HEAD] = (
                dqt[:, h * BLOCK:(h + 1) * BLOCK].T * scale)
        return 0

    lax.fori_loop(0, own, per_query_block, 0)

    def finish(r, _):
        rows = pl.ds(r * BLOCK, BLOCK)
        dkv_ref[0, rows, :] = (acc[0, rows, :] * scale).astype(dkv_ref.dtype)
        dkv_ref[1, rows, :] = acc[1, rows, :].astype(dkv_ref.dtype)
        return 0

    lax.fori_loop(0, blocks, finish, 0)


def local_grads(queries, out_grad, attn_out, log_norm, kv_all, block_layout, document_ids,
                block_order, sum_type):
    blocks = block_order.shape[0]
    total = kv_all.shape[1]
    starts = jnp.sum(
        (document_ids[None, :] < jnp.arange(DOCS, dtype=jnp.int32)[:, None]).astype(jnp.int32),
        axis=1)
    heads_of = document_ids.reshape(blocks, BLOCK)
    first_ids = heads_of[:, 0]
    first = jnp.sum(
        (document_ids[None, :] < first_ids[:, None]).astype(jnp.int32), axis=1) // BLOCK
    smem = pl.BlockSpec(memory_space=pltpu.SMEM)
    vmem = pl.BlockSpec(memory_space=pltpu.VMEM)
    heads = log_norm.shape[0]
    return pl.pallas_call(
        grads_kernel,
        out_shape=(
            jax.ShapeDtypeStruct(queries.shape, jnp.float32),
            jax.ShapeDtypeStruct((2, total, D_HEAD), sum_type),
        ),
        in_specs=[smem] * 4 + [vmem] * 6,
        out_specs=(vmem, vmem),
        scratch_shapes=[
            pltpu.VMEM((2, total, D_HEAD), jnp.float32),
            pltpu.SMEM((blocks,), jnp.int32),
            pltpu.VMEM((D_HEAD, heads * BLOCK), jnp.float32),
        ],
        name="grads",
    )(block_order, first, starts, block_layout.reshape(-1), heads_of,
      queries, out_grad, attn_out, log_norm, kv_all)


def place(cores, share):
    seq, head = lax.axis_index("seq"), lax.axis_index("head")
    return seq // cores, seq % cores, head // share, head % share


def remote(src, dst, send, recv, seq, head):
    copy = pltpu.make_async_remote_copy(
        src_ref=src, dst_ref=dst, send_sem=send, recv_sem=recv,
        device_id={"seq": seq, "head": head}, device_id_type=pl.DeviceIdType.MESH)
    copy.start()
    return copy


def greet(peers):
    barrier = pltpu.get_barrier_semaphore()
    for seq, head in peers:
        pl.semaphore_signal(barrier, inc=1, device_id={"seq": seq, "head": head},
                            device_id_type=pl.DeviceIdType.MESH)
    pl.semaphore_wait(barrier, len(peers))


def peers_of(deep, cores, kv_heads, share):
    z, c, g, x = place(cores, share)
    head = g * share + x
    seq = z * cores + c
    others = [(seq, (g + d) % kv_heads * share + x) for d in range(1, kv_heads)]
    others += [((z + d) % deep * cores + c, head) for d in range(1, deep)]
    others += [(seq, g * share + (x + d) % share) for d in range(1, share)]
    others += [(z * cores + (c + d) % cores, head) for d in range(1, cores)]
    return others


def gather_kernel(deep, cores, kv_heads, share, k_ref, v_ref, out, send, recv, recv_v, local):
    rows = k_ref.shape[0]
    z, c, g, x = place(cores, share)
    wide = kv_heads * share
    seq, head = z * cores + c, g * share + x
    greet(peers_of(deep, cores, kv_heads, share))
    sent = []

    def part(depth, core, group, lane):
        return (depth * cores + core) * wide + group * share + lane

    def span(index):
        return pl.ds(pl.multiple_of(index * rows, rows), rows)

    def push(src, dst, arrival, to_seq, to_head):
        sent.append(remote(src, dst, send.at[len(sent)], arrival, to_seq, to_head))

    def forward(index, to_seq, to_head):
        where = out.at[:, span(index), :]
        push(where, where, recv.at[index], to_seq, to_head)

    def arrived(index):
        where = out.at[:, span(index), :]
        pltpu.make_async_copy(where, where, recv.at[index]).wait()

    own = part(z, c, g, x)
    copies = []
    for n, ref in enumerate((k_ref, v_ref)):
        mine = ref.at[:, pl.ds(pl.multiple_of(g * D_HEAD, D_HEAD), D_HEAD)]
        copies.append(pltpu.make_async_copy(mine, out.at[n, span(own), :], local.at[n]))
        copies[-1].start()
    for d in range(1, kv_heads):
        other = (g + d) % kv_heads
        for n, ref in enumerate((k_ref, v_ref)):
            piece = ref.at[:, pl.ds(pl.multiple_of(other * D_HEAD, D_HEAD), D_HEAD)]
            arrival = recv.at[own] if n == 0 else recv_v.at[d - 1]
            push(piece, out.at[n, span(own), :], arrival, seq, other * share + x)
    for copy in copies:
        copy.wait()

    def to_core(index):
        for d in range(1, cores):
            forward(index, z * cores + (c + d) % cores, head)

    def to_sharers(index):
        for d in range(1, share):
            forward(index, seq, g * share + (x + d) % share)

    def to_deep(index):
        for d in range(1, deep):
            forward(index, (z + d) % deep * cores + c, head)

    def from_sharers(depth):
        for d in range(1, share):
            for j in range(kv_heads):
                index = part(depth, c, (g + j) % kv_heads, (x + d) % share)
                arrived(index)
                to_core(index)

    for j in range(kv_heads):
        index = part(z, c, (g + j) % kv_heads, x)
        if j:
            for n, sem in enumerate((recv.at[index], recv_v.at[kv_heads - j - 1])):
                where = out.at[n, span(index), :]
                pltpu.make_async_copy(where, where, sem).wait()
        to_deep(index)
        to_sharers(index)
        to_core(index)
    last = z
    for d in range(1, deep):
        depth = (z - d + deep) % deep
        for j in range(kv_heads):
            index = part(depth, c, (g + j) % kv_heads, x)
            arrived(index)
            to_sharers(index)
            to_core(index)
        from_sharers(last)
        last = depth
    from_sharers(last)
    for d in range(1, cores):
        for e in range(deep):
            for j in range(wide):
                arrived(part(e, (c + d) % cores, j // share, j % share))
    for copy in sent:
        copy.wait_send()


def gather(keys, values, seqs, heads, share):
    rows = keys.shape[0]
    kv_heads = heads // share
    cores = 2
    deep = seqs // cores
    parts = seqs * heads
    sends = 2 * (kv_heads - 1) + kv_heads * (deep - 1)
    sends += deep * kv_heads * (share - 1) + deep * heads * (cores - 1)
    vmem = pl.BlockSpec(memory_space=pltpu.VMEM)
    return pl.pallas_call(
        functools.partial(gather_kernel, deep, cores, kv_heads, share),
        out_shape=jax.ShapeDtypeStruct((2, parts * rows, D_HEAD), keys.dtype),
        in_specs=[vmem] * 2,
        out_specs=vmem,
        scratch_shapes=[
            pltpu.SemaphoreType.DMA((sends,)),
            pltpu.SemaphoreType.DMA((parts,)),
            pltpu.SemaphoreType.DMA((max(1, kv_heads - 1),)),
            pltpu.SemaphoreType.DMA((2,)),
        ],
        compiler_params=pltpu.CompilerParams(collective_id=0, has_side_effects=True),
        name="gather",
    )(keys, values)


def scatter_kernel(
    deep, cores, kv_heads, share, p_ref, dk_ref, dv_ref, core_in, kept, x_out, x_in, z_out, z_in,
    y_out, y_in, core_send, core_recv, x_send, x_recv, z_send, z_recv, y_send, y_recv,
):
    rows = dk_ref.shape[0]
    z, c, g, x = place(cores, share)
    wide = kv_heads * share
    seq, head = z * cores + c, g * share + x
    greet(peers_of(deep, cores, kv_heads, share))
    sent = []

    def depth_at(k):
        return (z + 1 + k) % deep

    def rows_of(depth, core):
        return pl.ds(pl.multiple_of((depth * cores + core) * wide * rows, wide * rows), wide * rows)

    core_copies = []
    for k in range(deep):
        for d in range(1, cores):
            to = (c + d) % cores
            slot = k * (cores - 1) + d - 1
            core_copies.append(remote(
                p_ref.at[:, rows_of(depth_at(k), to), :], core_in.at[slot],
                core_send.at[slot], core_recv.at[slot], z * cores + to, head))
    sent += core_copies

    def first_sum(k):
        base = (depth_at(k) * cores + c) * wide
        for d in range(1, cores):
            core_copies[k * (cores - 1) + d - 1].wait_recv()
        copies = []
        for e in range(share - 1, -1, -1):
            lane = (x + share - e) % share
            for j in range(kv_heads):
                inside = (j * share + lane) * rows
                here = pl.ds(pl.multiple_of(base * rows + inside, rows), rows)
                there = pl.ds(pl.multiple_of(inside, rows), rows)
                total = p_ref[:, here, :].astype(jnp.float32)
                for d in range(1, cores):
                    total += core_in[k * (cores - 1) + d - 1, :, there, :].astype(jnp.float32)
                if e:
                    x_out[k * (share - 1) + e - 1, :, j] = total.astype(jnp.bfloat16)
                else:
                    kept[k, :, j] = total
            if e:
                slot = k * (share - 1) + e - 1
                copies.append(remote(x_out.at[slot], x_in.at[slot], x_send.at[slot],
                                     x_recv.at[slot], seq, g * share + lane))
        sent.extend(copies)
        return copies

    def second_sum(k, copies):
        for copy in copies:
            copy.wait_recv()
        for j in range(kv_heads):
            total = kept[k, :, j]
            for e in range(1, share):
                total += x_in[k * (share - 1) + e - 1, :, j].astype(jnp.float32)
            if k < deep - 1:
                z_out[k, :, j] = total.astype(jnp.bfloat16)
            else:
                kept[k, :, j] = total
        if k < deep - 1:
            copy = remote(z_out.at[k], z_in.at[k], z_send.at[k], z_recv.at[k],
                          depth_at(k) * cores + c, head)
            sent.append(copy)
            return [copy]
        return []

    waiting, z_copies = None, []
    for k in range(deep):
        copies = first_sum(k)
        if waiting is not None:
            z_copies += second_sum(k - 1, waiting)
        waiting = copies
    z_copies += second_sum(deep - 1, waiting)
    for copy in z_copies:
        copy.wait_recv()
    y_copies = []
    for d in range(kv_heads - 1, -1, -1):
        group = (g + d) % kv_heads
        total = kept[deep - 1, :, group]
        for k in range(deep - 1):
            total += z_in[k, :, group].astype(jnp.float32)
        if d:
            y_out[d - 1] = total
            y_copies.append(remote(y_out.at[d - 1], y_in.at[g], y_send.at[d - 1],
                                   y_recv.at[d - 1], seq, group * share + x))
        else:
            y_in[g] = total
    sent += y_copies
    for d in range(1, kv_heads):
        where = y_in.at[(g - d + kv_heads) % kv_heads]
        pltpu.make_async_copy(where, where, y_recv.at[d - 1]).wait()
    for j in range(kv_heads):
        dk_ref[:, j * D_HEAD:(j + 1) * D_HEAD] = y_in[j, 0]
        dv_ref[:, j * D_HEAD:(j + 1) * D_HEAD] = y_in[j, 1]
    for copy in sent:
        copy.wait_send()


def scatter(partial, seqs, heads, share):
    kv_heads = heads // share
    cores = 2
    deep = seqs // cores
    rows = partial.shape[1] // (seqs * heads)
    vmem = pl.BlockSpec(memory_space=pltpu.VMEM)
    grad = jax.ShapeDtypeStruct((rows, kv_heads * D_HEAD), jnp.float32)
    piece = (2, kv_heads, rows, D_HEAD)
    crossing = max(1, share - 1)
    far = max(1, deep - 1)
    near = max(1, kv_heads - 1)
    return pl.pallas_call(
        functools.partial(scatter_kernel, deep, cores, kv_heads, share),
        out_shape=(grad, grad),
        in_specs=[vmem],
        out_specs=(vmem, vmem),
        scratch_shapes=[
            pltpu.VMEM((deep * (cores - 1), 2, heads * rows, D_HEAD), jnp.bfloat16),
            pltpu.VMEM((deep,) + piece, jnp.float32),
            pltpu.VMEM((deep * crossing,) + piece, jnp.bfloat16),
            pltpu.VMEM((deep * crossing,) + piece, jnp.bfloat16),
            pltpu.VMEM((far,) + piece, jnp.bfloat16),
            pltpu.VMEM((far,) + piece, jnp.bfloat16),
            pltpu.VMEM((near, 2, rows, D_HEAD), jnp.float32),
            pltpu.VMEM((kv_heads, 2, rows, D_HEAD), jnp.float32),
        ] + [pltpu.SemaphoreType.DMA((deep * (cores - 1),))] * 2
        + [pltpu.SemaphoreType.DMA((deep * crossing,))] * 2
        + [pltpu.SemaphoreType.DMA((far,))] * 2
        + [pltpu.SemaphoreType.DMA((near,))] * 2,
        compiler_params=pltpu.CompilerParams(collective_id=1, has_side_effects=True),
        name="scatter",
    )(partial)


def body(
    queries, keys, values, attn_out, out_grad, log_norm, block_layout, document_ids, block_order
):
    share = GROUP // log_norm.shape[0]
    seqs, heads = lax.axis_size("seq"), lax.axis_size("head")
    kv_all = gather(keys, values, seqs, heads, share)
    dq, dkv = local_grads(queries, out_grad, attn_out, log_norm, kv_all, block_layout,
                          document_ids, block_order, jnp.bfloat16)
    return (dq,) + tuple(scatter(dkv, seqs, heads, share))


def solution(mesh):
    in_specs = (
        P("seq", "head"),
        P(("seq", "head"), None),
        P(("seq", "head"), None),
        P("seq", "head"),
        P("seq", "head"),
        P("head", "seq"),
        P("head", None, None),
        P(),
        P(),
    )
    out_specs = (P("seq", "head"), P(("seq", "head"), None), P(("seq", "head"), None))
    return jax.shard_map(body, mesh=mesh, in_specs=in_specs, out_specs=out_specs, check_vma=False)
```

```python
import functools
import math

import jax
import jax.numpy as jnp
from jax import lax
from jax.experimental import pallas as pl
from jax.experimental.pallas import tpu as pltpu
from jax.sharding import PartitionSpec as P

D_HEAD = 128
GROUP = 4
BLOCK = 128
DOCS = 8
CHUNK = 4
LOG2E = math.log2(math.e)
NT = (((1,), (1,)), ((), ()))
TN = (((0,), (0,)), ((), ()))


def grads_kernel(
    order, layout, docs, q_ref, do_ref, o_ref, ln_ref, kv_ref,
    dq_ref, dkv_ref, acc, inverse, starts, dqt,
):
    heads = ln_ref.shape[0]
    blocks = order.shape[0]
    own = q_ref.shape[0] // BLOCK
    scale = D_HEAD ** -0.5
    me = lax.axis_index("seq")
    wide = heads * BLOCK

    def clear(r, _):
        inverse[order[r]] = r
        acc[:, pl.ds(r * BLOCK, BLOCK), :] = jnp.zeros((2, BLOCK, D_HEAD), jnp.float32)
        return 0

    for d in range(DOCS):
        starts[d] = jnp.sum(jnp.where(docs[...] < d, 1.0, 0.0)).astype(jnp.int32)
    lax.fori_loop(0, blocks, clear, 0)
    lane = lax.broadcasted_iota(jnp.int32, (1, wide), 1)
    sub = lax.broadcasted_iota(jnp.int32, (BLOCK, wide), 0)

    def per_query_block(i, _):
        rows = pl.ds(i * BLOCK, BLOCK)
        qb = order[me * own + i]
        ids = docs[pl.ds(qb, 1), :]
        low = jnp.zeros((1, BLOCK), jnp.int32)
        for d in range(1, DOCS):
            low = jnp.where(ids >= d, starts[d], low)
        low = jnp.concatenate([low] * heads, axis=1)
        high = qb * BLOCK + lane % BLOCK
        q2 = jnp.concatenate(
            [q_ref[rows, h * D_HEAD:(h + 1) * D_HEAD] for h in range(heads)], axis=0)
        do2 = jnp.concatenate(
            [do_ref[rows, h * D_HEAD:(h + 1) * D_HEAD] for h in range(heads)], axis=0)
        o2 = jnp.concatenate(
            [o_ref[rows, h * D_HEAD:(h + 1) * D_HEAD] for h in range(heads)], axis=0)
        product = do2.astype(jnp.float32) * o2.astype(jnp.float32)
        delta = jnp.sum(product.T, axis=0, keepdims=True)
        norm = jnp.concatenate([ln_ref[h:h + 1, rows] for h in range(heads)], axis=1) * LOG2E
        dqt[...] = jnp.zeros_like(dqt)
        begin = starts[jnp.min(ids.astype(jnp.float32)).astype(jnp.int32)] // BLOCK
        trips = (qb - begin + CHUNK) // CHUNK

        def per_chunk(t, _):
            slots, keeps, ks, vs = [], [], [], []
            for c in range(CHUNK):
                kb = begin + t * CHUNK + c
                held = jnp.minimum(kb, qb)
                slot = pl.multiple_of(inverse[held] * BLOCK, BLOCK)
                slots.append(slot)
                top = jnp.full((1, wide), -1, jnp.int32)
                for h in range(heads):
                    on = (layout[h, qb, held] == 1) & (kb <= qb)
                    limit = jnp.where(on, 1 << 30, -1)
                    top = jnp.where(lane // BLOCK == h, jnp.minimum(high, limit), top)
                keeps.append((sub >= low - held * BLOCK) & (sub <= top - held * BLOCK))
                ks.append(kv_ref[0, pl.ds(slot, BLOCK), :])
                vs.append(kv_ref[1, pl.ds(slot, BLOCK), :])
            k4 = jnp.concatenate(ks, axis=0)
            v4 = jnp.concatenate(vs, axis=0)
            keep = jnp.concatenate(keeps, axis=0)
            st = lax.dot_general(k4, q2, NT, preferred_element_type=jnp.float32)
            dpt = lax.dot_general(v4, do2, NT, preferred_element_type=jnp.float32)
            w = jnp.where(keep, jnp.exp2(st * (scale * LOG2E) - norm), 0.0)
            wl = w.astype(jnp.bfloat16)
            dv = jnp.dot(wl, do2, preferred_element_type=jnp.float32)
            ds = (w * (dpt - delta)).astype(jnp.bfloat16)
            dk = jnp.dot(ds, q2, preferred_element_type=jnp.float32)
            dqt[...] += lax.dot_general(k4, ds, TN, preferred_element_type=jnp.float32)
            for c in range(CHUNK):
                part = slice(c * BLOCK, (c + 1) * BLOCK)
                acc[0, pl.ds(slots[c], BLOCK), :] += dk[part]
                acc[1, pl.ds(slots[c], BLOCK), :] += dv[part]
            return 0

        lax.fori_loop(0, trips, per_chunk, 0)
        for h in range(heads):
            dq_ref[rows, h * D_HEAD:(h + 1) * D_HEAD] = (
                dqt[:, h * BLOCK:(h + 1) * BLOCK].T * scale)
        return 0

    lax.fori_loop(0, own, per_query_block, 0)

    def finish(r, _):
        rows = pl.ds(r * BLOCK, BLOCK)
        dkv_ref[0, rows, :] = (acc[0, rows, :] * scale).astype(dkv_ref.dtype)
        dkv_ref[1, rows, :] = acc[1, rows, :].astype(dkv_ref.dtype)
        return 0

    lax.fori_loop(0, blocks, finish, 0)


def local_grads(queries, out_grad, attn_out, log_norm, kv_all, block_layout, document_ids,
                block_order, sum_type):
    blocks = block_order.shape[0]
    total = kv_all.shape[1]
    smem = pl.BlockSpec(memory_space=pltpu.SMEM)
    vmem = pl.BlockSpec(memory_space=pltpu.VMEM)
    heads = log_norm.shape[0]
    return pl.pallas_call(
        grads_kernel,
        out_shape=(
            jax.ShapeDtypeStruct(queries.shape, jnp.float32),
            jax.ShapeDtypeStruct((2, total, D_HEAD), sum_type),
        ),
        in_specs=[smem] * 2 + [vmem] * 6,
        out_specs=(vmem, vmem),
        scratch_shapes=[
            pltpu.VMEM((2, total, D_HEAD), jnp.float32),
            pltpu.SMEM((blocks,), jnp.int32),
            pltpu.SMEM((DOCS,), jnp.int32),
            pltpu.VMEM((D_HEAD, heads * BLOCK), jnp.float32),
        ],
        compiler_params=pltpu.CompilerParams(
            vmem_limit_bytes=8 * total * D_HEAD * 2 + (10 << 20)),
        name="grads",
    )(block_order, block_layout, document_ids.reshape(blocks, BLOCK),
      queries, out_grad, attn_out, log_norm, kv_all)


def place(cores, share):
    seq, head = lax.axis_index("seq"), lax.axis_index("head")
    return seq // cores, seq % cores, head // share, head % share


def remote(src, dst, send, recv, seq, head):
    copy = pltpu.make_async_remote_copy(
        src_ref=src, dst_ref=dst, send_sem=send, recv_sem=recv,
        device_id={"seq": seq, "head": head}, device_id_type=pl.DeviceIdType.MESH)
    copy.start()
    return copy


def greet(peers):
    barrier = pltpu.get_barrier_semaphore()
    for seq, head in peers:
        pl.semaphore_signal(barrier, inc=1, device_id={"seq": seq, "head": head},
                            device_id_type=pl.DeviceIdType.MESH)
    pl.semaphore_wait(barrier, len(peers))


def peers_of(deep, cores, kv_heads, share):
    z, c, g, x = place(cores, share)
    head = g * share + x
    seq = z * cores + c
    others = [(seq, (g + d) % kv_heads * share + x) for d in range(1, kv_heads)]
    others += [((z + d) % deep * cores + c, head) for d in range(1, deep)]
    others += [(seq, g * share + (x + d) % share) for d in range(1, share)]
    others += [(z * cores + (c + d) % cores, head) for d in range(1, cores)]
    return others


def gather_kernel(deep, cores, kv_heads, share, k_ref, v_ref, out, send, recv, recv_v, local):
    rows = k_ref.shape[0]
    z, c, g, x = place(cores, share)
    wide = kv_heads * share
    seq, head = z * cores + c, g * share + x
    greet(peers_of(deep, cores, kv_heads, share))
    sent = []

    def part(depth, core, group, lane):
        return (depth * cores + core) * wide + group * share + lane

    def span(index):
        return pl.ds(pl.multiple_of(index * rows, rows), rows)

    def push(src, dst, arrival, to_seq, to_head):
        sent.append(remote(src, dst, send.at[len(sent)], arrival, to_seq, to_head))

    def forward(index, to_seq, to_head):
        where = out.at[:, span(index), :]
        push(where, where, recv.at[index], to_seq, to_head)

    def arrived(index):
        where = out.at[:, span(index), :]
        pltpu.make_async_copy(where, where, recv.at[index]).wait()

    own = part(z, c, g, x)
    copies = []
    for n, ref in enumerate((k_ref, v_ref)):
        mine = ref.at[:, pl.ds(pl.multiple_of(g * D_HEAD, D_HEAD), D_HEAD)]
        copies.append(pltpu.make_async_copy(mine, out.at[n, span(own), :], local.at[n]))
        copies[-1].start()
    for d in range(1, kv_heads):
        other = (g + d) % kv_heads
        for n, ref in enumerate((k_ref, v_ref)):
            piece = ref.at[:, pl.ds(pl.multiple_of(other * D_HEAD, D_HEAD), D_HEAD)]
            arrival = recv.at[own] if n == 0 else recv_v.at[d - 1]
            push(piece, out.at[n, span(own), :], arrival, seq, other * share + x)
    for copy in copies:
        copy.wait()

    def to_core(index):
        for d in range(1, cores):
            forward(index, z * cores + (c + d) % cores, head)

    def to_sharers(index):
        for d in range(1, share):
            forward(index, seq, g * share + (x + d) % share)

    def to_deep(index):
        for d in range(1, deep):
            forward(index, (z + d) % deep * cores + c, head)

    def from_sharers(depth):
        for d in range(1, share):
            for j in range(kv_heads):
                index = part(depth, c, (g + j) % kv_heads, (x + d) % share)
                arrived(index)
                to_core(index)

    for j in range(kv_heads):
        index = part(z, c, (g + j) % kv_heads, x)
        if j:
            for n, sem in enumerate((recv.at[index], recv_v.at[kv_heads - j - 1])):
                where = out.at[n, span(index), :]
                pltpu.make_async_copy(where, where, sem).wait()
        to_deep(index)
        to_sharers(index)
        to_core(index)
    last = z
    for d in range(1, deep):
        depth = (z - d + deep) % deep
        for j in range(kv_heads):
            index = part(depth, c, (g + j) % kv_heads, x)
            arrived(index)
            to_sharers(index)
            to_core(index)
        from_sharers(last)
        last = depth
    from_sharers(last)
    for d in range(1, cores):
        for e in range(deep):
            for j in range(wide):
                arrived(part(e, (c + d) % cores, j // share, j % share))
    for copy in sent:
        copy.wait_send()


def gather(keys, values, seqs, heads, share):
    rows = keys.shape[0]
    kv_heads = heads // share
    cores = 2
    deep = seqs // cores
    parts = seqs * heads
    sends = 2 * (kv_heads - 1) + kv_heads * (deep - 1)
    sends += deep * kv_heads * (share - 1) + deep * heads * (cores - 1)
    vmem = pl.BlockSpec(memory_space=pltpu.VMEM)
    return pl.pallas_call(
        functools.partial(gather_kernel, deep, cores, kv_heads, share),
        out_shape=jax.ShapeDtypeStruct((2, parts * rows, D_HEAD), keys.dtype),
        in_specs=[vmem] * 2,
        out_specs=vmem,
        scratch_shapes=[
            pltpu.SemaphoreType.DMA((sends,)),
            pltpu.SemaphoreType.DMA((parts,)),
            pltpu.SemaphoreType.DMA((max(1, kv_heads - 1),)),
            pltpu.SemaphoreType.DMA((2,)),
        ],
        compiler_params=pltpu.CompilerParams(collective_id=0, has_side_effects=True,
            vmem_limit_bytes=2 * parts * rows * D_HEAD * 2 + (3 << 20)),
        name="gather",
    )(keys, values)


def scatter_kernel(
    deep, cores, kv_heads, share, p_ref, y_in, core_in, kept, x_out, x_in, z_out, z_in,
    y_out, core_send, core_recv, x_send, x_recv, z_send, z_recv, y_send, y_recv,
):
    rows = y_in.shape[2]
    z, c, g, x = place(cores, share)
    wide = kv_heads * share
    seq, head = z * cores + c, g * share + x
    greet(peers_of(deep, cores, kv_heads, share))
    sent = []

    def depth_at(k):
        return (z + 1 + k) % deep

    def rows_of(depth, core):
        return pl.ds(pl.multiple_of((depth * cores + core) * wide * rows, wide * rows), wide * rows)

    core_copies = []
    for k in range(deep):
        for d in range(1, cores):
            to = (c + d) % cores
            slot = k * (cores - 1) + d - 1
            core_copies.append(remote(
                p_ref.at[:, rows_of(depth_at(k), to), :], core_in.at[slot],
                core_send.at[slot], core_recv.at[slot], z * cores + to, head))
    sent += core_copies

    def first_sum(k):
        base = (depth_at(k) * cores + c) * wide
        for d in range(1, cores):
            core_copies[k * (cores - 1) + d - 1].wait_recv()
        copies = []
        for e in range(share - 1, -1, -1):
            lane = (x + share - e) % share
            for j in range(kv_heads):
                inside = (j * share + lane) * rows
                here = pl.ds(pl.multiple_of(base * rows + inside, rows), rows)
                there = pl.ds(pl.multiple_of(inside, rows), rows)
                total = p_ref[:, here, :].astype(jnp.float32)
                for d in range(1, cores):
                    total += core_in[k * (cores - 1) + d - 1, :, there, :].astype(jnp.float32)
                if e:
                    x_out[k * (share - 1) + e - 1, :, j] = total.astype(jnp.bfloat16)
                else:
                    kept[k, :, j] = total
            if e:
                slot = k * (share - 1) + e - 1
                copies.append(remote(x_out.at[slot], x_in.at[slot], x_send.at[slot],
                                     x_recv.at[slot], seq, g * share + lane))
        sent.extend(copies)
        return copies

    def second_sum(k, copies):
        for copy in copies:
            copy.wait_recv()
        for j in range(kv_heads):
            total = kept[k, :, j]
            for e in range(1, share):
                total += x_in[k * (share - 1) + e - 1, :, j].astype(jnp.float32)
            if k < deep - 1:
                z_out[k, :, j] = total.astype(jnp.bfloat16)
            else:
                kept[k, :, j] = total
        if k < deep - 1:
            copy = remote(z_out.at[k], z_in.at[k], z_send.at[k], z_recv.at[k],
                          depth_at(k) * cores + c, head)
            sent.append(copy)
            return [copy]
        return []

    waiting, z_copies = None, []
    for k in range(deep):
        copies = first_sum(k)
        if waiting is not None:
            z_copies += second_sum(k - 1, waiting)
        waiting = copies
    z_copies += second_sum(deep - 1, waiting)
    for copy in z_copies:
        copy.wait_recv()
    y_copies = []
    for d in range(kv_heads - 1, -1, -1):
        group = (g + d) % kv_heads
        total = kept[deep - 1, :, group]
        for k in range(deep - 1):
            total += z_in[k, :, group].astype(jnp.float32)
        if d:
            y_out[d - 1] = total
            y_copies.append(remote(y_out.at[d - 1], y_in.at[g], y_send.at[d - 1],
                                   y_recv.at[d - 1], seq, group * share + x))
        else:
            y_in[g] = total
    sent += y_copies
    for d in range(1, kv_heads):
        where = y_in.at[(g - d + kv_heads) % kv_heads]
        pltpu.make_async_copy(where, where, y_recv.at[d - 1]).wait()
    for copy in sent:
        copy.wait_send()


def lay_kernel(y_in, dk_ref, dv_ref):
    for j in range(y_in.shape[0]):
        dk_ref[:, j * D_HEAD:(j + 1) * D_HEAD] = y_in[j, 0]
        dv_ref[:, j * D_HEAD:(j + 1) * D_HEAD] = y_in[j, 1]


def scatter(partial, seqs, heads, share):
    kv_heads = heads // share
    cores = 2
    deep = seqs // cores
    rows = partial.shape[1] // (seqs * heads)
    vmem = pl.BlockSpec(memory_space=pltpu.VMEM)
    grad = jax.ShapeDtypeStruct((rows, kv_heads * D_HEAD), jnp.float32)
    piece = (2, kv_heads, rows, D_HEAD)
    crossing = max(1, share - 1)
    far = max(1, deep - 1)
    near = max(1, kv_heads - 1)
    merged = pl.pallas_call(
        functools.partial(scatter_kernel, deep, cores, kv_heads, share),
        out_shape=jax.ShapeDtypeStruct((kv_heads, 2, rows, D_HEAD), jnp.float32),
        in_specs=[vmem],
        out_specs=vmem,
        scratch_shapes=[
            pltpu.VMEM((deep * (cores - 1), 2, heads * rows, D_HEAD), jnp.bfloat16),
            pltpu.VMEM((deep,) + piece, jnp.float32),
            pltpu.VMEM((deep * crossing,) + piece, jnp.bfloat16),
            pltpu.VMEM((deep * crossing,) + piece, jnp.bfloat16),
            pltpu.VMEM((far,) + piece, jnp.bfloat16),
            pltpu.VMEM((far,) + piece, jnp.bfloat16),
            pltpu.VMEM((near, 2, rows, D_HEAD), jnp.float32),
        ] + [pltpu.SemaphoreType.DMA((deep * (cores - 1),))] * 2
        + [pltpu.SemaphoreType.DMA((deep * crossing,))] * 2
        + [pltpu.SemaphoreType.DMA((far,))] * 2
        + [pltpu.SemaphoreType.DMA((near,))] * 2,
        compiler_params=pltpu.CompilerParams(collective_id=1, has_side_effects=True,
            vmem_limit_bytes=6 * partial.shape[1] * D_HEAD * 2 + (6 << 20)),
        name="scatter",
    )(partial)
    return pl.pallas_call(
        lay_kernel,
        out_shape=(grad, grad),
        in_specs=[vmem],
        out_specs=(vmem, vmem),
        compiler_params=pltpu.CompilerParams(vmem_limit_bytes=4 << 20),
        name="lay",
    )(merged)


def body(
    queries, keys, values, attn_out, out_grad, log_norm, block_layout, document_ids, block_order
):
    share = GROUP // log_norm.shape[0]
    seqs, heads = lax.axis_size("seq"), lax.axis_size("head")
    kv_all = gather(keys, values, seqs, heads, share)
    dq, dkv = local_grads(queries, out_grad, attn_out, log_norm, kv_all, block_layout,
                          document_ids, block_order, jnp.bfloat16)
    return (dq,) + tuple(scatter(dkv, seqs, heads, share))


def solution(mesh):
    in_specs = (
        P("seq", "head"),
        P(("seq", "head"), None),
        P(("seq", "head"), None),
        P("seq", "head"),
        P("seq", "head"),
        P("head", "seq"),
        P("head", None, None),
        P(),
        P(),
    )
    out_specs = (P("seq", "head"), P(("seq", "head"), None), P(("seq", "head"), None))
    return jax.shard_map(body, mesh=mesh, in_specs=in_specs, out_specs=out_specs, check_vma=False)
```

```python
import functools
import math

import jax
import jax.numpy as jnp
from jax import lax
from jax.experimental import pallas as pl
from jax.experimental.pallas import tpu as pltpu
from jax.sharding import PartitionSpec as P

D_HEAD = 128
GROUP = 4
BLOCK = 128
DOCS = 8
CHUNK = 4
LOG2E = math.log2(math.e)
NT = (((1,), (1,)), ((), ()))
TN = (((0,), (0,)), ((), ()))


def grads_kernel(
    order, layout, docs, q_ref, do_ref, o_ref, ln_ref, kv_ref,
    dq_ref, dkv_ref, acc, inverse, starts, dqt,
):
    heads = ln_ref.shape[0]
    blocks = order.shape[0]
    own = q_ref.shape[0] // BLOCK
    scale = D_HEAD ** -0.5
    me = lax.axis_index("seq")
    wide = heads * BLOCK

    def clear(r, _):
        inverse[order[r]] = r
        acc[:, pl.ds(r * BLOCK, BLOCK), :] = jnp.zeros((2, BLOCK, D_HEAD), jnp.float32)
        return 0

    for d in range(DOCS):
        starts[d] = jnp.sum(jnp.where(docs[...] < d, 1.0, 0.0)).astype(jnp.int32)
    lax.fori_loop(0, blocks, clear, 0)
    lane = lax.broadcasted_iota(jnp.int32, (1, wide), 1)
    sub = lax.broadcasted_iota(jnp.int32, (BLOCK, wide), 0)

    def per_query_block(i, _):
        rows = pl.ds(i * BLOCK, BLOCK)
        qb = order[me * own + i]
        ids = docs[pl.ds(qb, 1), :]
        low = jnp.zeros((1, BLOCK), jnp.int32)
        for d in range(1, DOCS):
            low = jnp.where(ids >= d, starts[d], low)
        low = jnp.concatenate([low] * heads, axis=1)
        high = qb * BLOCK + lane % BLOCK
        q2 = jnp.concatenate(
            [q_ref[rows, h * D_HEAD:(h + 1) * D_HEAD] for h in range(heads)], axis=0)
        do2 = jnp.concatenate(
            [do_ref[rows, h * D_HEAD:(h + 1) * D_HEAD] for h in range(heads)], axis=0)
        o2 = jnp.concatenate(
            [o_ref[rows, h * D_HEAD:(h + 1) * D_HEAD] for h in range(heads)], axis=0)
        product = do2.astype(jnp.float32) * o2.astype(jnp.float32)
        delta = jnp.sum(product.T, axis=0, keepdims=True)
        norm = jnp.concatenate([ln_ref[h:h + 1, rows] for h in range(heads)], axis=1) * LOG2E
        dqt[...] = jnp.zeros_like(dqt)
        begin = starts[jnp.min(ids.astype(jnp.float32)).astype(jnp.int32)] // BLOCK
        trips = (qb - begin + CHUNK) // CHUNK

        def per_chunk(t, _):
            slots, keeps, ks, vs = [], [], [], []
            for c in range(CHUNK):
                kb = begin + t * CHUNK + c
                held = jnp.minimum(kb, qb)
                slot = pl.multiple_of(inverse[held] * BLOCK, BLOCK)
                slots.append(slot)
                top = jnp.full((1, wide), -1, jnp.int32)
                for h in range(heads):
                    on = (layout[h, qb, held] == 1) & (kb <= qb)
                    limit = jnp.where(on, 1 << 30, -1)
                    top = jnp.where(lane // BLOCK == h, jnp.minimum(high, limit), top)
                keeps.append((sub >= low - held * BLOCK) & (sub <= top - held * BLOCK))
                ks.append(kv_ref[0, pl.ds(slot, BLOCK), :])
                vs.append(kv_ref[1, pl.ds(slot, BLOCK), :])
            k4 = jnp.concatenate(ks, axis=0)
            v4 = jnp.concatenate(vs, axis=0)
            keep = jnp.concatenate(keeps, axis=0)
            st = lax.dot_general(k4, q2, NT, preferred_element_type=jnp.float32)
            dpt = lax.dot_general(v4, do2, NT, preferred_element_type=jnp.float32)
            w = jnp.where(keep, jnp.exp2(st * (scale * LOG2E) - norm), 0.0)
            wl = w.astype(jnp.bfloat16)
            dv = jnp.dot(wl, do2, preferred_element_type=jnp.float32)
            ds = (w * (dpt - delta)).astype(jnp.bfloat16)
            dk = jnp.dot(ds, q2, preferred_element_type=jnp.float32)
            dqt[...] += lax.dot_general(k4, ds, TN, preferred_element_type=jnp.float32)
            for c in range(CHUNK):
                part = slice(c * BLOCK, (c + 1) * BLOCK)
                acc[0, pl.ds(slots[c], BLOCK), :] += dk[part]
                acc[1, pl.ds(slots[c], BLOCK), :] += dv[part]
            return 0

        lax.fori_loop(0, trips, per_chunk, 0)
        for h in range(heads):
            dq_ref[rows, h * D_HEAD:(h + 1) * D_HEAD] = (
                dqt[:, h * BLOCK:(h + 1) * BLOCK].T * scale)
        return 0

    lax.fori_loop(0, own, per_query_block, 0)

    def finish(r, _):
        rows = pl.ds(r * BLOCK, BLOCK)
        dkv_ref[0, rows, :] = (acc[0, rows, :] * scale).astype(dkv_ref.dtype)
        dkv_ref[1, rows, :] = acc[1, rows, :].astype(dkv_ref.dtype)
        return 0

    lax.fori_loop(0, blocks, finish, 0)


def local_grads(queries, out_grad, attn_out, log_norm, kv_all, block_layout, document_ids,
                block_order, sum_type):
    blocks = block_order.shape[0]
    total = kv_all.shape[1]
    smem = pl.BlockSpec(memory_space=pltpu.SMEM)
    vmem = pl.BlockSpec(memory_space=pltpu.VMEM)
    heads = log_norm.shape[0]
    return pl.pallas_call(
        grads_kernel,
        out_shape=(
            jax.ShapeDtypeStruct(queries.shape, jnp.float32),
            jax.ShapeDtypeStruct((2, total, D_HEAD), sum_type),
        ),
        in_specs=[smem] * 2 + [vmem] * 6,
        out_specs=(vmem, vmem),
        scratch_shapes=[
            pltpu.VMEM((2, total, D_HEAD), jnp.float32),
            pltpu.SMEM((blocks,), jnp.int32),
            pltpu.SMEM((DOCS,), jnp.int32),
            pltpu.VMEM((D_HEAD, heads * BLOCK), jnp.float32),
        ],
        compiler_params=pltpu.CompilerParams(
            vmem_limit_bytes=8 * total * D_HEAD * 2 + (10 << 20)),
        name="grads",
    )(block_order, block_layout, document_ids.reshape(blocks, BLOCK),
      queries, out_grad, attn_out, log_norm, kv_all)


def place(cores, share):
    seq, head = lax.axis_index("seq"), lax.axis_index("head")
    return seq // cores, seq % cores, head // share, head % share


def remote(src, dst, send, recv, seq, head):
    copy = pltpu.make_async_remote_copy(
        src_ref=src, dst_ref=dst, send_sem=send, recv_sem=recv,
        device_id={"seq": seq, "head": head}, device_id_type=pl.DeviceIdType.MESH)
    copy.start()
    return copy


def greet(peers):
    barrier = pltpu.get_barrier_semaphore()
    for seq, head in peers:
        pl.semaphore_signal(barrier, inc=1, device_id={"seq": seq, "head": head},
                            device_id_type=pl.DeviceIdType.MESH)
    pl.semaphore_wait(barrier, len(peers))


def peers_of(deep, cores, kv_heads, share):
    z, c, g, x = place(cores, share)
    head = g * share + x
    seq = z * cores + c
    others = [(seq, (g + d) % kv_heads * share + x) for d in range(1, kv_heads)]
    others += [((z + d) % deep * cores + c, head) for d in range(1, deep)]
    others += [(seq, g * share + (x + d) % share) for d in range(1, share)]
    others += [(z * cores + (c + d) % cores, head) for d in range(1, cores)]
    return others


def gather_kernel(deep, cores, kv_heads, share, k_ref, v_ref, out, send, recv, recv_v, local):
    rows = k_ref.shape[0]
    z, c, g, x = place(cores, share)
    wide = kv_heads * share
    seq, head = z * cores + c, g * share + x
    greet(peers_of(deep, cores, kv_heads, share))
    sent = []

    def part(depth, core, group, lane):
        return (depth * cores + core) * wide + group * share + lane

    def span(index):
        return pl.ds(pl.multiple_of(index * rows, rows), rows)

    def push(src, dst, arrival, to_seq, to_head, there=True):
        def copy(slot=len(sent)):
            return pltpu.make_async_remote_copy(
                src_ref=src, dst_ref=dst, send_sem=send.at[slot], recv_sem=arrival,
                device_id={"seq": to_seq, "head": to_head},
                device_id_type=pl.DeviceIdType.MESH)

        sent.append((there, copy))
        when(there, lambda: copy().start())

    def when(there, run):
        if there is True:
            run()
        else:
            pl.when(there)(run)

    def forward(index, to_seq, to_head, there=True):
        where = out.at[:, span(index), :]
        push(where, where, recv.at[index], to_seq, to_head, there)

    def arrived(index):
        where = out.at[:, span(index), :]
        pltpu.make_async_copy(where, where, recv.at[index]).wait()

    own = part(z, c, g, x)
    copies = []
    for n, ref in enumerate((k_ref, v_ref)):
        mine = ref.at[:, pl.ds(pl.multiple_of(g * D_HEAD, D_HEAD), D_HEAD)]
        copies.append(pltpu.make_async_copy(mine, out.at[n, span(own), :], local.at[n]))
        copies[-1].start()
    for d in range(1, kv_heads):
        other = (g + d) % kv_heads
        for n, ref in enumerate((k_ref, v_ref)):
            piece = ref.at[:, pl.ds(pl.multiple_of(other * D_HEAD, D_HEAD), D_HEAD)]
            arrival = recv.at[own] if n == 0 else recv_v.at[d - 1]
            push(piece, out.at[n, span(own), :], arrival, seq, other * share + x)
    for copy in copies:
        copy.wait()

    def to_core(index, there=True):
        for d in range(1, cores):
            forward(index, z * cores + (c + d) % cores, head, there)

    def to_sharers(index, there=True):
        for d in range(1, share):
            forward(index, seq, g * share + (x + d) % share, there)

    def onward(index, step, there):
        forward(index, (z + step) * cores + c, head, there)

    def from_sharers(depth, there=True):
        for d in range(1, share):
            for j in range(kv_heads):
                index = part(depth, c, (g + j) % kv_heads, (x + d) % share)
                when(there, functools.partial(arrived, index))
                to_core(index, there)

    for j in range(kv_heads):
        index = part(z, c, (g + j) % kv_heads, x)
        if j:
            for n, sem in enumerate((recv.at[index], recv_v.at[kv_heads - j - 1])):
                where = out.at[n, span(index), :]
                pltpu.make_async_copy(where, where, sem).wait()
        onward(index, 1, z + 1 < deep)
        onward(index, -1, z > 0)
        to_sharers(index)
        to_core(index)
    pending = [(z, True)]
    for d in range(1, deep):
        sides = ((z - d, 1, z - d >= 0), (z + d, -1, z + d < deep))
        for j in range(kv_heads):
            for depth, step, here in sides:
                index = part(depth, c, (g + j) % kv_heads, x)
                when(here, functools.partial(arrived, index))
                if d < deep - 1:
                    more = z + 1 < deep if step == 1 else z > 0
                    onward(index, step, here & more)
                to_sharers(index, here)
                to_core(index, here)
        for depth, there in pending:
            from_sharers(depth, there)
        pending = [(depth, here) for depth, _, here in sides]
    for depth, there in pending:
        from_sharers(depth, there)
    for d in range(1, cores):
        for e in range(deep):
            for j in range(wide):
                arrived(part(e, (c + d) % cores, j // share, j % share))
    for there, copy in sent:
        when(there, lambda: copy().wait_send())


def gather(keys, values, seqs, heads, share):
    rows = keys.shape[0]
    kv_heads = heads // share
    cores = 2
    deep = seqs // cores
    parts = seqs * heads
    hops = 2 * (deep - 1)
    sends = 2 * (kv_heads - 1) + kv_heads * (share + cores)
    sends += hops * kv_heads * (share + cores - 1)
    sends += (1 + hops) * kv_heads * (share - 1) * (cores - 1)
    vmem = pl.BlockSpec(memory_space=pltpu.VMEM)
    return pl.pallas_call(
        functools.partial(gather_kernel, deep, cores, kv_heads, share),
        out_shape=jax.ShapeDtypeStruct((2, parts * rows, D_HEAD), keys.dtype),
        in_specs=[vmem] * 2,
        out_specs=vmem,
        scratch_shapes=[
            pltpu.SemaphoreType.DMA((sends,)),
            pltpu.SemaphoreType.DMA((parts,)),
            pltpu.SemaphoreType.DMA((max(1, kv_heads - 1),)),
            pltpu.SemaphoreType.DMA((2,)),
        ],
        compiler_params=pltpu.CompilerParams(collective_id=0, has_side_effects=True,
            vmem_limit_bytes=2 * parts * rows * D_HEAD * 2 + (3 << 20)),
        name="gather",
    )(keys, values)


def scatter_kernel(
    deep, cores, kv_heads, share, p_ref, y_in, core_in, kept, x_out, x_in, z_out, z_in,
    y_out, core_send, core_recv, x_send, x_recv, z_send, z_recv, y_send, y_recv,
):
    rows = y_in.shape[2]
    z, c, g, x = place(cores, share)
    wide = kv_heads * share
    seq, head = z * cores + c, g * share + x
    greet(peers_of(deep, cores, kv_heads, share))
    sent = []

    def depth_at(k):
        return (z + 1 + k) % deep

    def rows_of(depth, core):
        return pl.ds(pl.multiple_of((depth * cores + core) * wide * rows, wide * rows), wide * rows)

    core_copies = []
    for k in range(deep):
        for d in range(1, cores):
            to = (c + d) % cores
            slot = k * (cores - 1) + d - 1
            core_copies.append(remote(
                p_ref.at[:, rows_of(depth_at(k), to), :], core_in.at[slot],
                core_send.at[slot], core_recv.at[slot], z * cores + to, head))
    sent += core_copies

    def first_sum(k):
        base = (depth_at(k) * cores + c) * wide
        for d in range(1, cores):
            core_copies[k * (cores - 1) + d - 1].wait_recv()
        copies = []
        for e in range(share - 1, -1, -1):
            lane = (x + share - e) % share
            for j in range(kv_heads):
                inside = (j * share + lane) * rows
                here = pl.ds(pl.multiple_of(base * rows + inside, rows), rows)
                there = pl.ds(pl.multiple_of(inside, rows), rows)
                total = p_ref[:, here, :].astype(jnp.float32)
                for d in range(1, cores):
                    total += core_in[k * (cores - 1) + d - 1, :, there, :].astype(jnp.float32)
                if e:
                    x_out[k * (share - 1) + e - 1, :, j] = total.astype(jnp.bfloat16)
                else:
                    kept[k, :, j] = total
            if e:
                slot = k * (share - 1) + e - 1
                copies.append(remote(x_out.at[slot], x_in.at[slot], x_send.at[slot],
                                     x_recv.at[slot], seq, g * share + lane))
        sent.extend(copies)
        return copies

    def second_sum(k, copies):
        for copy in copies:
            copy.wait_recv()
        for j in range(kv_heads):
            total = kept[k, :, j]
            for e in range(1, share):
                total += x_in[k * (share - 1) + e - 1, :, j].astype(jnp.float32)
            if k < deep - 1:
                z_out[k, :, j] = total.astype(jnp.bfloat16)
            else:
                kept[k, :, j] = total
        if k < deep - 1:
            copy = remote(z_out.at[k], z_in.at[k], z_send.at[k], z_recv.at[k],
                          depth_at(k) * cores + c, head)
            sent.append(copy)
            return [copy]
        return []

    waiting, z_copies = None, []
    for k in range(deep):
        copies = first_sum(k)
        if waiting is not None:
            z_copies += second_sum(k - 1, waiting)
        waiting = copies
    z_copies += second_sum(deep - 1, waiting)
    for copy in z_copies:
        copy.wait_recv()
    y_copies = []
    for d in range(kv_heads - 1, -1, -1):
        group = (g + d) % kv_heads
        total = kept[deep - 1, :, group]
        for k in range(deep - 1):
            total += z_in[k, :, group].astype(jnp.float32)
        if d:
            y_out[d - 1] = total
            y_copies.append(remote(y_out.at[d - 1], y_in.at[g], y_send.at[d - 1],
                                   y_recv.at[d - 1], seq, group * share + x))
        else:
            y_in[g] = total
    sent += y_copies
    for d in range(1, kv_heads):
        where = y_in.at[(g - d + kv_heads) % kv_heads]
        pltpu.make_async_copy(where, where, y_recv.at[d - 1]).wait()
    for copy in sent:
        copy.wait_send()


def lay_kernel(y_in, dk_ref, dv_ref):
    for j in range(y_in.shape[0]):
        dk_ref[:, j * D_HEAD:(j + 1) * D_HEAD] = y_in[j, 0]
        dv_ref[:, j * D_HEAD:(j + 1) * D_HEAD] = y_in[j, 1]


def scatter(partial, seqs, heads, share):
    kv_heads = heads // share
    cores = 2
    deep = seqs // cores
    rows = partial.shape[1] // (seqs * heads)
    vmem = pl.BlockSpec(memory_space=pltpu.VMEM)
    grad = jax.ShapeDtypeStruct((rows, kv_heads * D_HEAD), jnp.float32)
    piece = (2, kv_heads, rows, D_HEAD)
    crossing = max(1, share - 1)
    far = max(1, deep - 1)
    near = max(1, kv_heads - 1)
    merged = pl.pallas_call(
        functools.partial(scatter_kernel, deep, cores, kv_heads, share),
        out_shape=jax.ShapeDtypeStruct((kv_heads, 2, rows, D_HEAD), jnp.float32),
        in_specs=[vmem],
        out_specs=vmem,
        scratch_shapes=[
            pltpu.VMEM((deep * (cores - 1), 2, heads * rows, D_HEAD), jnp.bfloat16),
            pltpu.VMEM((deep,) + piece, jnp.float32),
            pltpu.VMEM((deep * crossing,) + piece, jnp.bfloat16),
            pltpu.VMEM((deep * crossing,) + piece, jnp.bfloat16),
            pltpu.VMEM((far,) + piece, jnp.bfloat16),
            pltpu.VMEM((far,) + piece, jnp.bfloat16),
            pltpu.VMEM((near, 2, rows, D_HEAD), jnp.float32),
        ] + [pltpu.SemaphoreType.DMA((deep * (cores - 1),))] * 2
        + [pltpu.SemaphoreType.DMA((deep * crossing,))] * 2
        + [pltpu.SemaphoreType.DMA((far,))] * 2
        + [pltpu.SemaphoreType.DMA((near,))] * 2,
        compiler_params=pltpu.CompilerParams(collective_id=1, has_side_effects=True,
            vmem_limit_bytes=6 * partial.shape[1] * D_HEAD * 2 + (6 << 20)),
        name="scatter",
    )(partial)
    return pl.pallas_call(
        lay_kernel,
        out_shape=(grad, grad),
        in_specs=[vmem],
        out_specs=(vmem, vmem),
        compiler_params=pltpu.CompilerParams(vmem_limit_bytes=4 << 20),
        name="lay",
    )(merged)


def body(
    queries, keys, values, attn_out, out_grad, log_norm, block_layout, document_ids, block_order
):
    share = GROUP // log_norm.shape[0]
    seqs, heads = lax.axis_size("seq"), lax.axis_size("head")
    kv_all = gather(keys, values, seqs, heads, share)
    dq, dkv = local_grads(queries, out_grad, attn_out, log_norm, kv_all, block_layout,
                          document_ids, block_order, jnp.bfloat16)
    return (dq,) + tuple(scatter(dkv, seqs, heads, share))


def solution(mesh):
    in_specs = (
        P("seq", "head"),
        P(("seq", "head"), None),
        P(("seq", "head"), None),
        P("seq", "head"),
        P("seq", "head"),
        P("head", "seq"),
        P("head", None, None),
        P(),
        P(),
    )
    out_specs = (P("seq", "head"), P(("seq", "head"), None), P(("seq", "head"), None))
    return jax.shard_map(body, mesh=mesh, in_specs=in_specs, out_specs=out_specs, check_vma=False)
```
